32 devices in a mesh: rep: 2 (over x), tp: 4 (over z), dp: 4 (over y, core).
Axes of the slice: x: 2, y: 2, z: 4, core: 2. Of those that a mesh axis runs over, the one named last changes fastest.
Arguments:
- grad_partial: float32 [8, 8, 768, 3072], P(('rep', 'dp'), None, None, 'tp'), parts along dimension 0
- momentum: float32 [16, 768, 3072], P('rep', 'dp', 'tp'), parts along dimension 0
- weight: float32 [16, 768, 3072], P('rep', 'dp', 'tp'), parts along dimension 0
- learn_rate: float32 [16], P('rep'), parts along dimension 0
- decay_rate: float32 [], replicated
Outputs:
- output 1: float32 [16, 768, 3072], P('rep', 'dp', 'tp'), parts along dimension 0
- output 2: float32 [16, 768, 3072], P('rep', 'dp', 'tp'), parts along dimension 0
- output 3: bfloat16 [16, 768, 3072], P('rep', None, 'tp'), parts along dimension 0
There are 2 independent parts. The reference program is written for one: setup_inputs(seed, part) draws one part's arguments, and reference() takes and returns one part's arrays. A program takes and returns all parts, laid end to end along the dimension named above; an argument that names none is the same for every part.
All inputs are finite; a program needn't handle non-finite values.
Results may differ from the reference program's by a relative error of at most 0.0113773.
Values are sent between devices in bfloat16 or wider.
A program may use at most 1 GiB of HBM per device.

```python
import math
import jax
import jax.numpy as jnp
from jax import lax

DP_SIZE = 4
MATS = 8
ROWS = 768
COLS = 3072

MOMENTUM = 0.95
NS_STEPS = 5
COEF_A = 3.4445
COEF_B = -4.7750
COEF_C = 2.0315
NORM_EPS = 1e-7
OUT_SCALE = 0.2 * math.sqrt(max(ROWS, COLS))


def setup_inputs(seed: int = 0, part: int = 0) -> dict:
    part_key = jax.random.fold_in(jax.random.key(seed), part)
    key_grad, key_scale, key_mom, key_weight, key_rate = jax.random.split(part_key, 5)
    key_decay = jax.random.key(seed + 1)
    dev_scale = jax.random.uniform(key_scale, (DP_SIZE, 1, 1, 1), minval=0.5, maxval=2.0)
    grad_partial = jax.random.normal(key_grad, (DP_SIZE, MATS, ROWS, COLS)) * dev_scale * math.sqrt(DP_SIZE)
    momentum = jax.random.normal(key_mom, (MATS, ROWS, COLS))
    weight = 0.25 * jax.random.normal(key_weight, (MATS, ROWS, COLS))
    learn_rate = jax.random.uniform(key_rate, (MATS,), minval=0.1, maxval=1.0)
    decay_rate = jax.random.uniform(key_decay, (), minval=0.2, maxval=0.5)
    return {
        "grad_partial": grad_partial.astype(jnp.float32),
        "momentum": momentum.astype(jnp.float32),
        "weight": weight.astype(jnp.float32),
        "learn_rate": learn_rate.astype(jnp.float32),
        "decay_rate": decay_rate.astype(jnp.float32),
    }


def orthogonalize(update):
    upd_f32 = update.astype(jnp.float32)
    norm_val = jnp.sqrt(jnp.sum(upd_f32 * upd_f32))
    x_cur = (upd_f32 / (norm_val + NORM_EPS)).astype(jnp.bfloat16)
    if ROWS > COLS:
        x_cur = x_cur.T
    for step_idx in range(NS_STEPS):
        gram_mat = jnp.dot(x_cur, x_cur.T, preferred_element_type=jnp.float32).astype(jnp.bfloat16)
        gram_sq = jnp.dot(gram_mat, gram_mat, preferred_element_type=jnp.float32)
        poly_mat = (COEF_B * gram_mat.astype(jnp.float32) + COEF_C * gram_sq).astype(jnp.bfloat16)
        prod_mat = jnp.dot(poly_mat, x_cur, preferred_element_type=jnp.float32)
        x_cur = (COEF_A * x_cur.astype(jnp.float32) + prod_mat).astype(jnp.bfloat16)
    if ROWS > COLS:
        x_cur = x_cur.T
    return x_cur


def reference(grad_partial, momentum, weight, learn_rate, decay_rate):
    grad_mean = jnp.mean(grad_partial, axis=0)
    mom_new = MOMENTUM * momentum + grad_mean
    update = (grad_mean + MOMENTUM * mom_new).astype(jnp.bfloat16)
    ortho_mat = lax.map(orthogonalize, update)
    rate_col = learn_rate[:, None, None]
    weight_new = weight - rate_col * (OUT_SCALE * ortho_mat.astype(jnp.float32) + decay_rate * weight)
    return mom_new, weight_new, weight_new.astype(jnp.bfloat16)
```

```python
import functools
import math
import jax
import jax.numpy as jnp
from jax import lax
from jax.experimental import pallas as pl
from jax.experimental.pallas import tpu as pltpu
from jax.sharding import PartitionSpec as P

MOMENTUM = 0.95
NS_STEPS = 5
COEF_A = 3.4445
COEF_B = -4.7750
COEF_C = 2.0315
NORM_EPS = 1e-7
MESH = pl.DeviceIdType.MESH
F32 = jnp.float32
BF16 = jnp.bfloat16

LAG_IN = 2
LAG_OUT = 2


def owner_of(j):
    half = j // 4
    tp = (j % 2) * (3 - 2 * half) + half
    y = ((j + 1) // 2) % 2
    return tp, y


def matrix_of(tp, y):
    half = ((tp + 1) // 2) % 2
    par = tp // 2
    return 4 * half + par + 2 * ((y + par) % 2)


def kernel(cfg, lr_ref, decay_ref, grad, mom_in, wt_in, mom_o, wt_o, wb_o,
           own, rcv, yr, mom, wt, ub, x, ga, gb, xr, wb, wr,
           s_own, s_mom, s_wt, s_c2s, s_c2r, s_ys, s_yr, s_us, s_ur, s_fs, s_fr, s_xs, s_xr,
           s_mo, s_wo, s_wl, s_ps, s_pr, s_gs, s_gr, s_fl, s_qs, s_qr):
    mats, rows, cols, ncol, out_scale, inv_dp = cfg
    full_rows = 4 * rows
    tp = lax.axis_index("tp")
    dp = lax.axis_index("dp")
    y = dp // 2
    c = dp % 2
    oy = 1 - y
    oc = 1 - c
    dp_core = y * 2 + oc
    dp_y = oy * 2 + c
    mine = matrix_of(tp, y)

    def rowq(q):
        return pl.ds(pl.multiple_of(q * rows, rows), rows)

    def colq(t):
        return pl.ds(pl.multiple_of(t * cols, cols), cols)

    def remote(src, dst, ss, rs, tp_id, dp_id):
        return pltpu.make_async_remote_copy(
            src_ref=src, dst_ref=dst, send_sem=ss, recv_sem=rs,
            device_id={"tp": tp_id, "dp": dp_id}, device_id_type=MESH)

    def own_copy(j, q):
        return pltpu.make_async_copy(grad.at[j, rowq(q * 2 + c), :], own.at[j, q], s_own.at[j, q])

    def mom_copy(j):
        return pltpu.make_async_copy(mom_in.at[j], mom.at[j], s_mom.at[j])

    def wt_copy(j):
        return pltpu.make_async_copy(wt_in.at[j], wt.at[j], s_wt.at[j])

    def core_send(j, q):
        return remote(grad.at[j, rowq(q * 2 + oc), :], rcv.at[j, q], s_c2s.at[j, q], s_c2r.at[j, q], tp, dp_core)

    barrier = pltpu.get_barrier_semaphore()
    pl.semaphore_signal(barrier, inc=1, device_id={"tp": tp, "dp": dp_core}, device_id_type=MESH)
    for k in range(1, 8):
        tgt = (tp * 2 + y + k) % 8
        pl.semaphore_signal(barrier, inc=1, device_id={"tp": tgt // 2, "dp": (tgt % 2) * 2 + c}, device_id_type=MESH)
    for q in range(2):
        own_copy(0, q).start()
    pl.semaphore_wait(barrier, 8)

    @pl.loop(0, mats)
    def _(j):
        for q in range(2):
            core_send(j, q).start()

        @pl.when(j > 0)
        def _():
            for q in range(2):
                own_copy(j, q).start()
        mom_copy(j).start()

    @pl.loop(0, mats)
    def _(j):
        wt_copy(j).start()

    def y_send(j):
        return remote(own.at[j, oy], yr.at[j], s_ys.at[j], s_yr.at[j], tp, dp_y)

    def sum_cores(j):
        for q in range(2):
            own_copy(j, q).wait()
            core_send(j, q).wait_recv()

        @pl.loop(0, rows, step=16)
        def _(r):
            rr = pl.ds(pl.multiple_of(r, 16), 16)
            own[j, oy, rr, :] = own[j, oy, rr, :] + rcv[j, oy, rr, :]
        y_send(j).start()

    def u_send(j, tp_id, dp_id):
        return remote(ub.at[j], x.at[rowq(dp), colq(tp)], s_us.at[j], s_ur.at[y, tp], tp_id, dp_id)

    def sum_y(j):
        y_send(j).wait_recv()
        mom_copy(j).wait()

        @pl.loop(0, rows, step=16)
        def _(r):
            rr = pl.ds(pl.multiple_of(r, 16), 16)
            g = (own[j, y, rr, :] + rcv[j, y, rr, :] + yr[j, rr, :]) * inv_dp
            m = MOMENTUM * mom[j, rr, :] + g
            mom[j, rr, :] = m
            ub[j, rr, :] = (g + MOMENTUM * m).astype(BF16)
        pltpu.make_async_copy(mom.at[j], mom_o.at[j], s_mo.at[j]).start()
        otp, oyy = owner_of(j)

        @pl.when(mine == j)
        def _():
            x[rowq(dp), colq(tp)] = ub[j]

        @pl.when(mine != j)
        def _():
            u_send(j, otp, oyy * 2 + c).start()

    def piece(yy, tt):
        return remote(ub.at[0], x.at[rowq(yy * 2 + c), colq(tt)], s_us.at[0], s_ur.at[yy, tt], tp, dp_core)

    def x_fwd(q):
        blk = x.at[rowq(q * 2 + c), :]
        return remote(blk, blk, s_fs.at[q], s_fr.at[q], tp, dp_core)

    def x_fwd_in(q):
        blk = x.at[rowq(q * 2 + oc), :]
        return remote(blk, blk, s_fs.at[q], s_fr.at[q], tp, dp_core)

    def gather_x():
        for q in range(2):
            for t in range(4):
                @pl.when(jnp.logical_or(y != q, tp != t))
                def _():
                    piece(q, t).wait_recv()
            x_fwd(q).start()
        for q in range(2):
            x_fwd_in(q).wait_recv()
        for q in range(2):
            x_fwd(q).wait_send()

        def body(i, acc):
            rr = pl.ds(pl.multiple_of(i * 16, 16), 16)
            v = x[rr, :].astype(F32)
            v = v * v
            for t in range(ncol // cols):
                acc = acc + v[:, t * cols:(t + 1) * cols]
            return acc
        acc = lax.fori_loop(0, full_rows // 16, body, jnp.zeros((16, cols), F32))
        total = jnp.sum(acc, axis=(0, 1), keepdims=True)
        inv = 1.0 / (jnp.sqrt(total) + NORM_EPS)

        @pl.loop(0, full_rows, step=16)
        def _(r):
            rr = pl.ds(pl.multiple_of(r, 16), 16)
            x[rr, :] = (x[rr, :].astype(F32) * inv).astype(BF16)

    def ns_step():
        blk = min(256, full_rows)

        @pl.loop(0, full_rows, step=blk)
        def _(r):
            rr = pl.ds(pl.multiple_of(r, blk), blk)
            ga[rr, :] = lax.dot_general(x[rr, :], x[...], (((1,), (1,)), ((), ())),
                                        preferred_element_type=F32).astype(BF16)

        @pl.loop(0, full_rows, step=blk)
        def _(r):
            rr = pl.ds(pl.multiple_of(r, blk), blk)
            sq = jnp.dot(ga[rr, :], ga[...], preferred_element_type=F32)
            gb[rr, :] = (COEF_B * ga[rr, :].astype(F32) + COEF_C * sq).astype(BF16)

        cblk = min(512, ncol)

        @pl.loop(0, ncol, step=cblk)
        def _(r):
            rr = pl.ds(pl.multiple_of(r, cblk), cblk)
            prod = jnp.dot(gb[...], x[:, rr], preferred_element_type=F32)
            x[:, rr] = (COEF_A * x[:, rr].astype(F32) + prod).astype(BF16)

    def x_send(q, t):
        return remote(x.at[rowq(q * 2 + c), colq(t)], xr.at[mine], s_xs.at[q, t], s_xr.at[mine], t, q * 2 + c)

    def x_recv(m):
        return remote(x.at[rowq(c), colq(0)], xr.at[m], s_xs.at[0, 0], s_xr.at[m], tp, dp_core)

    def send_back():
        for q in range(2):
            for t in range(4):
                @pl.when(jnp.logical_or(y != q, tp != t))
                def _():
                    x_send(q, t).start()

                @pl.when(jnp.logical_and(y == q, tp == t))
                def _():
                    xr[mine] = x[rowq(q * 2 + c), colq(t)]

    def wb_local(m):
        return pltpu.make_async_copy(wb.at[m], wb_o.at[m, rowq(dp), :], s_wl.at[m])

    def wb_core(m):
        return remote(wb.at[m], wb_o.at[m, rowq(dp), :], s_ps.at[m], s_pr.at[m], tp, dp_core)

    def wb_core_in(m):
        return remote(wb.at[m], wb_o.at[m, rowq(dp_core), :], s_ps.at[m], s_pr.at[m], tp, dp_core)

    def wb_y(m):
        return remote(wb.at[m], wr.at[m], s_gs.at[m], s_gr.at[m], tp, dp_y)

    def update(m):
        @pl.when(mine != m)
        def _():
            x_recv(m).wait_recv()
        wt_copy(m).wait()
        rate = lr_ref[m]
        decay = decay_ref[0]

        @pl.loop(0, rows, step=16)
        def _(r):
            rr = pl.ds(pl.multiple_of(r, 16), 16)
            w = wt[m, rr, :]
            w = w - rate * (out_scale * xr[m, rr, :].astype(F32) + decay * w)
            wt[m, rr, :] = w
            wb[m, rr, :] = w.astype(BF16)
        wb_y(m).start()
        wb_core(m).start()
        wb_local(m).start()
        pltpu.make_async_copy(wt.at[m], wt_o.at[m], s_wo.at[m]).start()

    def fwd_local(m):
        return pltpu.make_async_copy(wr.at[m], wb_o.at[m, rowq(dp_y), :], s_fl.at[m])

    def fwd_core(m):
        return remote(wr.at[m], wb_o.at[m, rowq(dp_y), :], s_qs.at[m], s_qr.at[m], tp, dp_core)

    def fwd_core_in(m):
        return remote(wr.at[m], wb_o.at[m, rowq(oy * 2 + oc), :], s_qs.at[m], s_qr.at[m], tp, dp_core)

    def forward(m):
        wb_y(m).wait_recv()
        fwd_core(m).start()
        fwd_local(m).start()

    first_ns = mine + 1 + LAG_IN
    lag = 1 + LAG_IN + NS_STEPS + LAG_OUT

    @pl.loop(0, mats + lag + 1)
    def _(t):
        @pl.when(t < mats)
        def _():
            sum_cores(t)

        @pl.when(jnp.logical_and(t >= 1, t < mats + 1))
        def _():
            sum_y(t - 1)

        @pl.when(t == first_ns)
        def _():
            gather_x()

        @pl.when(jnp.logical_and(t >= first_ns, t < first_ns + NS_STEPS))
        def _():
            ns_step()

        @pl.when(t == first_ns + NS_STEPS - 1)
        def _():
            send_back()

        @pl.when(jnp.logical_and(t >= lag, t < mats + lag))
        def _():
            update(t - lag)

        @pl.when(t >= lag + 1)
        def _():
            forward(t - lag - 1)

    @pl.loop(0, mats)
    def _(j):
        for q in range(2):
            core_send(j, q).wait_send()
        y_send(j).wait_send()

        @pl.when(mine != j)
        def _():
            u_send(j, tp, dp_core).wait_send()
        pltpu.make_async_copy(mom.at[j], mom_o.at[j], s_mo.at[j]).wait()
        pltpu.make_async_copy(wt.at[j], wt_o.at[j], s_wo.at[j]).wait()
        wb_local(j).wait()
        wb_core(j).wait_send()
        wb_core_in(j).wait_recv()
        wb_y(j).wait_send()
        fwd_local(j).wait()
        fwd_core(j).wait_send()
        fwd_core_in(j).wait_recv()
    for q in range(2):
        for t in range(4):
            @pl.when(jnp.logical_or(y != q, tp != t))
            def _():
                x_send(q, t).wait_send()


def solution(mesh):
    dp_size = mesh.shape["dp"]
    tp_size = mesh.shape["tp"]

    def local_step(grad_local, mom_local, weight_local, learn_rate, decay_rate):
        mats, rows, cols = mom_local.shape
        ncol = cols * tp_size
        nrow = rows * dp_size
        cfg = (mats, rows, cols, ncol, 0.2 * math.sqrt(max(nrow, ncol)), 1.0 / dp_size)
        dma = pltpu.SemaphoreType.DMA
        smem = pl.BlockSpec(memory_space=pltpu.SMEM)
        hbm = pl.BlockSpec(memory_space=pl.ANY)
        return pl.pallas_call(
            functools.partial(kernel, cfg),
            out_shape=(jax.ShapeDtypeStruct((mats, rows, cols), F32),
                       jax.ShapeDtypeStruct((mats, rows, cols), F32),
                       jax.ShapeDtypeStruct((mats, nrow, cols), BF16)),
            in_specs=[smem, smem, hbm, hbm, hbm],
            out_specs=(hbm, hbm, hbm),
            scratch_shapes=[
                pltpu.VMEM((mats, 2, rows, cols), F32),
                pltpu.VMEM((mats, 2, rows, cols), F32),
                pltpu.VMEM((mats, rows, cols), F32),
                pltpu.VMEM((mats, rows, cols), F32),
                pltpu.VMEM((mats, rows, cols), F32),
                pltpu.VMEM((mats, rows, cols), BF16),
                pltpu.VMEM((nrow, ncol), BF16),
                pltpu.VMEM((nrow, nrow), BF16),
                pltpu.VMEM((nrow, nrow), BF16),
                pltpu.VMEM((mats, rows, cols), BF16),
                pltpu.VMEM((mats, rows, cols), BF16),
                pltpu.VMEM((mats, rows, cols), BF16),
                dma((mats, 2)), dma((mats,)), dma((mats,)),
                dma((mats, 2)), dma((mats, 2)),
                dma((mats,)), dma((mats,)),
                dma((mats,)), dma((2, tp_size)),
                dma((2,)), dma((2,)),
                dma((2, tp_size)), dma((mats,)),
                dma((mats,)), dma((mats,)), dma((mats,)),
                dma((mats,)), dma((mats,)), dma((mats,)), dma((mats,)),
                dma((mats,)), dma((mats,)), dma((mats,)),
            ],
            compiler_params=pltpu.CompilerParams(
                collective_id=0, has_side_effects=True, vmem_limit_bytes=66 * 1024 * 1024 - 2 ** 21),
            name="muon_step",
        )(learn_rate, decay_rate.reshape(1), grad_local[0], mom_local, weight_local)

    return jax.shard_map(
        local_step,
        mesh=mesh,
        in_specs=(P(("rep", "dp"), None, None, "tp"), P("rep", "dp", "tp"), P("rep", "dp", "tp"), P("rep"), P()),
        out_specs=(P("rep", "dp", "tp"), P("rep", "dp", "tp"), P("rep", None, "tp")),
        check_vma=False,
    )
```

```python
import functools
import math
import jax
import jax.numpy as jnp
from jax import lax
from jax.experimental import pallas as pl
from jax.experimental.pallas import tpu as pltpu
from jax.sharding import PartitionSpec as P

MOMENTUM = 0.95
NS_STEPS = 5
COEF_A = 3.4445
COEF_B = -4.7750
COEF_C = 2.0315
NORM_EPS = 1e-7
MESH = pl.DeviceIdType.MESH
F32 = jnp.float32
BF16 = jnp.bfloat16

LAG_IN = 3
LAG_UPD = 13
LAG_FWD = 3
HELD, GUARD = 1, 6
FAST_SLOTS = 6
AHEAD = 2


def owner_of(j):
    half = j // 4
    tp = (j % 2) * (3 - 2 * half) + half
    y = ((j + 1) // 2) % 2
    return tp, y


def matrix_of(tp, y):
    half = ((tp + 1) // 2) % 2
    par = tp // 2
    return 4 * half + par + 2 * ((y + par) % 2)


def kernel(cfg, lr_ref, decay_ref, grad, mom_in, wt_in, mom_o, wt_o, wb_o,
           own, rcv, yr, mom, wt, ub, x, ga, gb, uf, acc, xr, wb, wr,
           s_own, s_mom, s_wt, s_c2s, s_c2r, s_ys, s_yr, s_us, s_ur, s_fs, s_fr, s_xs, s_xr,
           s_hs, s_hr, s_vs, s_mo, s_wo, s_wl, s_ps, s_pr, s_gs, s_gr, s_fl, s_qs, s_qr, s_go):
    mats, rows, cols, ncol, out_scale, inv_dp = cfg
    full_rows = 4 * rows
    tp = lax.axis_index("tp")
    dp = lax.axis_index("dp")
    y = dp // 2
    c = dp % 2
    oy = 1 - y
    oc = 1 - c
    dp_core = y * 2 + oc
    dp_y = oy * 2 + c
    mine = matrix_of(tp, y)

    def rowq(q):
        return pl.ds(pl.multiple_of(q * rows, rows), rows)

    def colq(t):
        return pl.ds(pl.multiple_of(t * cols, cols), cols)

    def remote(src, dst, ss, rs, tp_id, dp_id):
        return pltpu.make_async_remote_copy(
            src_ref=src, dst_ref=dst, send_sem=ss, recv_sem=rs,
            device_id={"tp": tp_id, "dp": dp_id}, device_id_type=MESH)

    def own_copy(j, q):
        return pltpu.make_async_copy(grad.at[j, rowq(q * 2 + c), :], own.at[j, q], s_own.at[j, q])

    def mom_copy(j):
        return pltpu.make_async_copy(mom_in.at[j], mom.at[j], s_mom.at[j])

    def wt_copy(j):
        return pltpu.make_async_copy(wt_in.at[j], wt.at[j], s_wt.at[j])

    def core_send(j, q):
        return remote(grad.at[j, rowq(q * 2 + oc), :], rcv.at[j, q], s_c2s.at[j, q], s_c2r.at[j, q], tp, dp_core)

    barrier = pltpu.get_barrier_semaphore()
    pl.semaphore_signal(barrier, inc=1, device_id={"tp": tp, "dp": dp_core}, device_id_type=MESH)
    for k in range(1, 8):
        tgt = (tp * 2 + y + k) % 8
        pl.semaphore_signal(barrier, inc=1, device_id={"tp": tgt // 2, "dp": (tgt % 2) * 2 + c}, device_id_type=MESH)
    own_copy(0, oy).start()
    pl.semaphore_wait(barrier, 8)

    def issue(j, first):
        core_send(j, oy).start()
        if not first:
            own_copy(j, oy).start()
        core_send(j, y).start()
        own_copy(j, y).start()
        mom_copy(j).start()

    for j in range(AHEAD):
        issue(j, j == 0)

    def y_send(j):
        return remote(own.at[j, oy], yr.at[j], s_ys.at[j], s_yr.at[j], tp, dp_y)

    def sum_cores(j):
        own_copy(j, oy).wait()
        core_send(j, oy).wait_recv()

        @pl.loop(0, rows, step=16)
        def _(r):
            rr = pl.ds(pl.multiple_of(r, 16), 16)
            own[j, oy, rr, :] = own[j, oy, rr, :] + rcv[j, oy, rr, :]
        y_send(j).start()

    def u_send(j, tp_id, dp_id):
        return remote(ub.at[j], x.at[rowq(dp), colq(tp)], s_us.at[j], s_ur.at[y, tp], tp_id, dp_id)

    def sum_y(j):
        own_copy(j, y).wait()
        core_send(j, y).wait_recv()
        mom_copy(j).wait()
        y_send(j).wait_recv()

        @pl.loop(0, rows, step=16)
        def _(r):
            rr = pl.ds(pl.multiple_of(r, 16), 16)
            g = (own[j, y, rr, :] + rcv[j, y, rr, :] + yr[j, rr, :]) * inv_dp
            m = MOMENTUM * mom[j, rr, :] + g
            mom[j, rr, :] = m
            ub[j, rr, :] = (g + MOMENTUM * m).astype(BF16)
        pltpu.make_async_copy(mom.at[j], mom_o.at[j], s_mo.at[j]).start()
        wt_copy(j).start()
        otp, oyy = owner_of(j)

        @pl.when(mine == j)
        def _():
            x[rowq(dp), colq(tp)] = ub[j]

        @pl.when(jnp.logical_and(mine != j, y == oyy))
        def _():
            u_send(j, otp, dp).start()

        @pl.when(y != oyy)
        def _():
            u_cross(j).start()

    def u_cross(j):
        return remote(ub.at[j], uf.at[j], s_hs.at[j], s_hr.at[j], tp, dp_y)

    def u_pass(j, tp_id, dp_id):
        return remote(uf.at[j], x.at[rowq(dp_y), colq(tp)], s_vs.at[j], s_ur.at[oy, tp], tp_id, dp_id)

    def hop(j):
        otp, oyy = owner_of(j)

        @pl.when(y == oyy)
        def _():
            u_cross(j).wait_recv()

            @pl.when(mine == j)
            def _():
                x[rowq(dp_y), colq(tp)] = uf[j]

            @pl.when(mine != j)
            def _():
                u_pass(j, otp, dp).start()

    def piece(yy, tt):
        return remote(ub.at[0], x.at[rowq(yy * 2 + c), colq(tt)], s_us.at[0], s_ur.at[yy, tt], tp, dp_core)

    def x_fwd(q, t):
        blk = x.at[rowq(q * 2 + c), colq(t)]
        return remote(blk, blk, s_fs.at[q, t], s_fr.at[q, t], tp, dp_core)

    def x_fwd_in(q, t):
        blk = x.at[rowq(q * 2 + oc), colq(t)]
        return remote(blk, blk, s_fs.at[q, t], s_fr.at[q, t], tp, dp_core)

    def add_squares(q, t):
        def body(i, carry):
            v = x[pl.ds(pl.multiple_of(q * rows + i * 16, 16), 16), colq(t)].astype(F32)
            return carry + v * v
        acc[...] = lax.fori_loop(0, rows // 16, body, acc[...])

    def gather_x():
        acc[...] = jnp.zeros_like(acc)
        for q in (y, oy):
            for k in range(4):
                t = (tp + k) % 4
                if k > 0:
                    piece(q, t).wait_recv()
                x_fwd(q, t).start()
                add_squares(q * 2 + c, t)
        for q in (y, oy):
            for k in range(4):
                t = (tp + k) % 4
                x_fwd_in(q, t).wait_recv()
                add_squares(q * 2 + oc, t)
        for q in range(2):
            for t in range(4):
                x_fwd(q, t).wait_send()
        total = jnp.sum(acc[...], axis=(0, 1), keepdims=True)
        inv = 1.0 / (jnp.sqrt(total) + NORM_EPS)

        @pl.loop(0, full_rows, step=16)
        def _(r):
            rr = pl.ds(pl.multiple_of(r, 16), 16)
            x[rr, :] = (x[rr, :].astype(F32) * inv).astype(BF16)

    blk = min(256, full_rows // 2)
    strips = full_rows // blk

    def mirror(dst, i, strip):
        for k in range(i + 1, strips):
            dst[k * blk:(k + 1) * blk, i * blk:(i + 1) * blk] = strip[:, (k - i) * blk:(k - i + 1) * blk].T

    def gram():
        for i in range(strips):
            lo = i * blk
            strip = lax.dot_general(x[lo:lo + blk, :], x[lo:, :], (((1,), (1,)), ((), ())),
                                    preferred_element_type=F32).astype(BF16)
            ga[lo:lo + blk, lo:] = strip
            mirror(ga, i, strip)

    def ns_step():
        gram()
        for i in range(strips):
            lo = i * blk
            sq = jnp.dot(ga[lo:lo + blk, :], ga[:, lo:], preferred_element_type=F32)
            strip = (COEF_B * ga[lo:lo + blk, lo:].astype(F32) + COEF_C * sq).astype(BF16)
            gb[lo:lo + blk, lo:] = strip
            mirror(gb, i, strip)
        cblk = ncol // 2

        @pl.loop(0, ncol, step=cblk)
        def _(r):
            rr = pl.ds(pl.multiple_of(r, cblk), cblk)
            prod = jnp.dot(gb[...], x[:, rr], preferred_element_type=F32)
            x[:, rr] = (COEF_A * x[:, rr].astype(F32) + prod).astype(BF16)

    def ns_last():
        gram()
        for q in range(2):
            part = ga[rowq(q * 2 + c), :]
            sq = jnp.dot(part, ga[...], preferred_element_type=F32)
            gb[q * rows:(q + 1) * rows, :] = (COEF_B * part.astype(F32) + COEF_C * sq).astype(BF16)

        @pl.loop(0, 4)
        def _(i):
            t = i + (3 - 2 * i) * (1 - tp // 2)
            prod = jnp.dot(gb[:2 * rows, :], x[:, colq(t)], preferred_element_type=F32)
            for q in range(2):
                rr = rowq(q * 2 + c)
                x[rr, colq(t)] = (COEF_A * x[rr, colq(t)].astype(F32)
                                  + prod[q * rows:(q + 1) * rows, :]).astype(BF16)
            @pl.when(mine != HELD)
            def _():
                for q in range(2):
                    send_back(q, t)

    def x_send(q, t):
        return remote(x.at[rowq(q * 2 + c), colq(t)], xr.at[mine], s_xs.at[q, t], s_xr.at[mine], t, q * 2 + c)

    def x_recv(m):
        return remote(x.at[rowq(c), colq(0)], xr.at[m], s_xs.at[0, 0], s_xr.at[m], tp, dp_core)

    def send_back(q, t):
        @pl.when(jnp.logical_or(y != q, tp != t))
        def _():
            x_send(q, t).start()

        @pl.when(jnp.logical_and(y == q, tp == t))
        def _():
            xr[mine] = x[rowq(q * 2 + c), colq(t)]

    def wb_local(m):
        return pltpu.make_async_copy(wb.at[m], wb_o.at[m, rowq(dp), :], s_wl.at[m])

    def wb_core(m):
        return remote(wb.at[m], wb_o.at[m, rowq(dp), :], s_ps.at[m], s_pr.at[m], tp, dp_core)

    def wb_core_in(m):
        return remote(wb.at[m], wb_o.at[m, rowq(dp_core), :], s_ps.at[m], s_pr.at[m], tp, dp_core)

    def wb_y(m):
        return remote(wb.at[m], wr.at[m], s_gs.at[m], s_gr.at[m], tp, dp_y)

    def update(m):
        @pl.when(mine != m)
        def _():
            x_recv(m).wait_recv()
        wt_copy(m).wait()
        rate = lr_ref[m]
        decay = decay_ref[0]

        @pl.loop(0, rows, step=16)
        def _(r):
            rr = pl.ds(pl.multiple_of(r, 16), 16)
            w = wt[m, rr, :]
            w = w - rate * (out_scale * xr[m, rr, :].astype(F32) + decay * w)
            wt[m, rr, :] = w
            wb[m, rr, :] = w.astype(BF16)
        wb_y(m).start()
        wb_core(m).start()
        wb_local(m).start()
        pltpu.make_async_copy(wt.at[m], wt_o.at[m], s_wo.at[m]).start()

    def fwd_local(m):
        return pltpu.make_async_copy(wr.at[m], wb_o.at[m, rowq(dp_y), :], s_fl.at[m])

    def fwd_core(m):
        return remote(wr.at[m], wb_o.at[m, rowq(dp_y), :], s_qs.at[m], s_qr.at[m], tp, dp_core)

    def fwd_core_in(m):
        return remote(wr.at[m], wb_o.at[m, rowq(oy * 2 + oc), :], s_qs.at[m], s_qr.at[m], tp, dp_core)

    def forward(m):
        wb_y(m).wait_recv()
        fwd_core(m).start()
        fwd_local(m).start()

    first_ns = mine + 1 + LAG_IN

    def steps_before(t):
        done = t - first_ns + jnp.maximum(jnp.minimum(t, FAST_SLOTS) - first_ns, 0)
        return jnp.minimum(jnp.maximum(done, 0), NS_STEPS)


    sum_cores(0)

    @pl.loop(0, mats + LAG_UPD + LAG_FWD)
    def _(t):
        @pl.when(t < mats - AHEAD)
        def _():
            issue(t + AHEAD, False)

        @pl.when(jnp.logical_and(t >= 1, t < mats + 1))
        def _():
            sum_y(t - 1)

        @pl.when(t < mats - 1)
        def _():
            sum_cores(t + 1)

        @pl.when(jnp.logical_and(t >= 2, t < mats + 2))
        def _():
            hop(t - 2)

        @pl.when(jnp.logical_and(t == mats + 2, mine == HELD))
        def _():
            pl.semaphore_wait(s_go, 1)

            @pl.loop(0, 4)
            def _(i):
                k = i + (3 - 2 * i) * (1 - tp // 2)
                for q in range(2):
                    send_back(q, k)

        @pl.when(jnp.logical_and(t >= LAG_UPD, t < mats + LAG_UPD))
        def _():
            update(t - LAG_UPD)

        @pl.when(t >= LAG_UPD + LAG_FWD)
        def _():
            forward(t - LAG_UPD - LAG_FWD)

        @pl.when(t == first_ns)
        def _():
            gather_x()

            @pl.when(mine == GUARD)
            def _():
                htp, hy = owner_of(HELD)
                pl.semaphore_signal(s_go, inc=1, device_id={"tp": htp, "dp": hy * 2 + c}, device_id_type=MESH)

        begin = steps_before(t)
        end = steps_before(t + 1)

        @pl.loop(begin, jnp.minimum(end, NS_STEPS - 1))
        def _(i):
            ns_step()

        @pl.when(jnp.logical_and(begin < NS_STEPS, end == NS_STEPS))
        def _():
            ns_last()

    @pl.loop(0, mats)
    def _(j):
        for q in range(2):
            core_send(j, q).wait_send()
        y_send(j).wait_send()

        otp, oyy = owner_of(j)

        @pl.when(jnp.logical_and(mine != j, y == oyy))
        def _():
            u_send(j, tp, dp_core).wait_send()
            u_pass(j, tp, dp_core).wait_send()

        @pl.when(y != oyy)
        def _():
            u_cross(j).wait_send()
        pltpu.make_async_copy(mom.at[j], mom_o.at[j], s_mo.at[j]).wait()
        pltpu.make_async_copy(wt.at[j], wt_o.at[j], s_wo.at[j]).wait()
        wb_local(j).wait()
        wb_core(j).wait_send()
        wb_core_in(j).wait_recv()
        wb_y(j).wait_send()
        fwd_local(j).wait()
        fwd_core(j).wait_send()
        fwd_core_in(j).wait_recv()
    for q in range(2):
        for t in range(4):
            @pl.when(jnp.logical_or(y != q, tp != t))
            def _():
                x_send(q, t).wait_send()


def solution(mesh):
    dp_size = mesh.shape["dp"]
    tp_size = mesh.shape["tp"]

    def local_step(grad_local, mom_local, weight_local, learn_rate, decay_rate):
        mats, rows, cols = mom_local.shape
        ncol = cols * tp_size
        nrow = rows * dp_size
        cfg = (mats, rows, cols, ncol, 0.2 * math.sqrt(max(nrow, ncol)), 1.0 / dp_size)
        dma = pltpu.SemaphoreType.DMA
        smem = pl.BlockSpec(memory_space=pltpu.SMEM)
        hbm = pl.BlockSpec(memory_space=pl.ANY)
        return pl.pallas_call(
            functools.partial(kernel, cfg),
            out_shape=(jax.ShapeDtypeStruct((mats, rows, cols), F32),
                       jax.ShapeDtypeStruct((mats, rows, cols), F32),
                       jax.ShapeDtypeStruct((mats, nrow, cols), BF16)),
            in_specs=[smem, smem, hbm, hbm, hbm],
            out_specs=(hbm, hbm, hbm),
            scratch_shapes=[
                pltpu.VMEM((mats, 2, rows, cols), F32),
                pltpu.VMEM((mats, 2, rows, cols), F32),
                pltpu.VMEM((mats, rows, cols), F32),
                pltpu.VMEM((mats, rows, cols), F32),
                pltpu.VMEM((mats, rows, cols), F32),
                pltpu.VMEM((mats, rows, cols), BF16),
                pltpu.VMEM((nrow, ncol), BF16),
                pltpu.VMEM((nrow, nrow), BF16),
                pltpu.VMEM((nrow, nrow), BF16),
                pltpu.VMEM((mats, rows, cols), BF16),
                pltpu.VMEM((16, cols), F32),
                pltpu.VMEM((mats, rows, cols), BF16),
                pltpu.VMEM((mats, rows, cols), BF16),
                pltpu.VMEM((mats, rows, cols), BF16),
                dma((mats, 2)), dma((mats,)), dma((mats,)),
                dma((mats, 2)), dma((mats, 2)),
                dma((mats,)), dma((mats,)),
                dma((mats,)), dma((2, tp_size)),
                dma((2, tp_size)), dma((2, tp_size)),
                dma((2, tp_size)), dma((mats,)),
                dma((mats,)), dma((mats,)), dma((mats,)),
                dma((mats,)), dma((mats,)), dma((mats,)),
                dma((mats,)), dma((mats,)), dma((mats,)), dma((mats,)),
                dma((mats,)), dma((mats,)), dma((mats,)),
                pltpu.SemaphoreType.REGULAR,
            ],
            compiler_params=pltpu.CompilerParams(
                collective_id=0, has_side_effects=True, vmem_limit_bytes=66 * 1024 * 1024 - 2 ** 21),
            name="muon_step",
        )(learn_rate, decay_rate.reshape(1), grad_local[0], mom_local, weight_local)

    return jax.shard_map(
        local_step,
        mesh=mesh,
        in_specs=(P(("rep", "dp"), None, None, "tp"), P("rep", "dp", "tp"), P("rep", "dp", "tp"), P("rep"), P()),
        out_specs=(P("rep", "dp", "tp"), P("rep", "dp", "tp"), P("rep", None, "tp")),
        check_vma=False,
    )
```

```python
import functools
import math
import jax
import jax.numpy as jnp
from jax import lax
from jax.experimental import pallas as pl
from jax.experimental.pallas import tpu as pltpu
from jax.sharding import PartitionSpec as P

MOMENTUM = 0.95
NS_STEPS = 5
COEF_A = 3.4445
COEF_B = -4.7750
COEF_C = 2.0315
NORM_EPS = 1e-7
MESH = pl.DeviceIdType.MESH
F32 = jnp.float32
BF16 = jnp.bfloat16

OWNERS = ((2, 0), (1, 1), (3, 1), (0, 0), (0, 1), (3, 0), (1, 0), (2, 1))
DIRECT = ()
CROSS_SLOT = 9
AHEAD = 2
VMEM_MIB = 44
FAST_SLOTS = (6, 9)
EARLY = 10
LATE = 13
LAG_FWD = 3


def owner_of(j):
    tp, y = 0, 0
    for k, (tp_k, y_k) in enumerate(OWNERS):
        tp = tp + jnp.where(j == k, tp_k, 0)
        y = y + jnp.where(j == k, y_k, 0)
    return tp, y


def matrix_of(tp, y):
    mine = 0
    for k, (tp_k, y_k) in enumerate(OWNERS):
        mine = mine + jnp.where(jnp.logical_and(tp == tp_k, y == y_k), k, 0)
    return mine


def kernel(cfg, lr_ref, decay_ref, grad, mom_in, wt_in, mom, wt, wb,
           own, rcv, yr, ub, x, ga, gb, uf, acc, xr,
           s_own, s_mom, s_wt, s_c2s, s_c2r, s_ys, s_yr, s_us, s_ur, s_fs, s_fr, s_xs, s_xr,
           s_hs, s_hr, s_vs, s_ps, s_pr, s_gs, s_gr, s_qs, s_qr):
    mats, rows, cols, ncol, out_scale, inv_dp = cfg
    full_rows = 4 * rows
    tp = lax.axis_index("tp")
    dp = lax.axis_index("dp")
    y = dp // 2
    c = dp % 2
    oy = 1 - y
    oc = 1 - c
    dp_core = y * 2 + oc
    dp_y = oy * 2 + c
    mine = matrix_of(tp, y)

    def rowq(q):
        return pl.ds(pl.multiple_of(q * rows, rows), rows)

    def colq(t):
        return pl.ds(pl.multiple_of(t * cols, cols), cols)

    def remote(src, dst, ss, rs, tp_id, dp_id):
        return pltpu.make_async_remote_copy(
            src_ref=src, dst_ref=dst, send_sem=ss, recv_sem=rs,
            device_id={"tp": tp_id, "dp": dp_id}, device_id_type=MESH)

    def own_copy(j, q):
        return pltpu.make_async_copy(grad.at[j, rowq(q * 2 + c), :], own.at[j, q], s_own.at[j, q])

    def mom_copy(j):
        return pltpu.make_async_copy(mom_in.at[j], mom.at[j], s_mom.at[j])

    def wt_copy(j):
        return pltpu.make_async_copy(wt_in.at[j], wt.at[j], s_wt.at[j])

    def core_send(j, q):
        return remote(grad.at[j, rowq(q * 2 + oc), :], rcv.at[j, q], s_c2s.at[j, q], s_c2r.at[j, q], tp, dp_core)

    barrier = pltpu.get_barrier_semaphore()
    pl.semaphore_signal(barrier, inc=1, device_id={"tp": tp, "dp": dp_core}, device_id_type=MESH)
    for k in range(1, 8):
        tgt = (tp * 2 + y + k) % 8
        pl.semaphore_signal(barrier, inc=1, device_id={"tp": tgt // 2, "dp": (tgt % 2) * 2 + c}, device_id_type=MESH)
    own_copy(0, oy).start()
    pl.semaphore_wait(barrier, 8)

    def issue(j, first):
        core_send(j, oy).start()
        if not first:
            own_copy(j, oy).start()
        core_send(j, y).start()
        own_copy(j, y).start()
        mom_copy(j).start()

    for j in range(AHEAD):
        issue(j, j == 0)

    def y_send(j):
        return remote(own.at[j, oy], yr.at[j], s_ys.at[j], s_yr.at[j], tp, dp_y)

    def sum_cores(j):
        own_copy(j, oy).wait()
        core_send(j, oy).wait_recv()

        @pl.loop(0, rows, step=16)
        def _(r):
            rr = pl.ds(pl.multiple_of(r, 16), 16)
            own[j, oy, rr, :] = own[j, oy, rr, :] + rcv[j, oy, rr, :]
        y_send(j).start()

    def is_direct(j):
        hit = 0
        for k, tp_k, c_k in DIRECT:
            hit = hit + jnp.where(jnp.logical_and(j == k, jnp.logical_and(tp == tp_k, c == c_k)), 1, 0)
        return hit

    def u_send(j, tp_id, dp_id):
        return remote(ub.at[j], x.at[rowq(dp), colq(tp)], s_us.at[j], s_ur.at[y, tp], tp_id, dp_id)

    def sum_y(j):
        own_copy(j, y).wait()
        core_send(j, y).wait_recv()
        mom_copy(j).wait()
        y_send(j).wait_recv()

        @pl.loop(0, rows, step=16)
        def _(r):
            rr = pl.ds(pl.multiple_of(r, 16), 16)
            g = (own[j, y, rr, :] + rcv[j, y, rr, :] + yr[j, rr, :]) * inv_dp
            m = MOMENTUM * mom[j, rr, :] + g
            mom[j, rr, :] = m
            ub[j, rr, :] = (g + MOMENTUM * m).astype(BF16)
        wt_copy(j).start()
        otp, oyy = owner_of(j)

        @pl.when(mine == j)
        def _():
            x[rowq(dp), colq(tp)] = ub[j]

        @pl.when(jnp.logical_and(mine != j, y == oyy))
        def _():
            u_send(j, otp, dp).start()

        direct = is_direct(j)

        @pl.when(jnp.logical_and(y != oyy, direct == 1))
        def _():
            u_send(j, otp, oyy * 2 + c).start()

        @pl.when(jnp.logical_and(y != oyy, direct == 0))
        def _():
            u_cross(j).start()

    def u_cross(j):
        return remote(ub.at[j], uf.at[j], s_hs.at[j], s_hr.at[j], tp, dp_y)

    def u_pass(j, tp_id, dp_id):
        return remote(uf.at[j], x.at[rowq(dp_y), colq(tp)], s_vs.at[j], s_ur.at[oy, tp], tp_id, dp_id)

    def hop(j):
        otp, oyy = owner_of(j)

        @pl.when(jnp.logical_and(y == oyy, is_direct(j) == 0))
        def _():
            u_cross(j).wait_recv()

            @pl.when(mine == j)
            def _():
                x[rowq(dp_y), colq(tp)] = uf[j]

            @pl.when(mine != j)
            def _():
                u_pass(j, otp, dp).start()

    def piece(yy, tt):
        return remote(ub.at[0], x.at[rowq(yy * 2 + c), colq(tt)], s_us.at[0], s_ur.at[yy, tt], tp, dp_core)

    def x_fwd(q, t):
        blk = x.at[rowq(q * 2 + c), colq(t)]
        return remote(blk, blk, s_fs.at[q, t], s_fr.at[q, t], tp, dp_core)

    def x_fwd_in(q, t):
        blk = x.at[rowq(q * 2 + oc), colq(t)]
        return remote(blk, blk, s_fs.at[q, t], s_fr.at[q, t], tp, dp_core)

    def add_squares(q, t):
        def body(i, carry):
            v = x[pl.ds(pl.multiple_of(q * rows + i * 16, 16), 16), colq(t)].astype(F32)
            return carry + v * v
        acc[...] = lax.fori_loop(0, rows // 16, body, acc[...])

    def gather_x():
        acc[...] = jnp.zeros_like(acc)
        for q in (y, oy):
            for k in range(4):
                t = (tp + k) % 4
                if k > 0:
                    piece(q, t).wait_recv()
                x_fwd(q, t).start()
                add_squares(q * 2 + c, t)
        for q in (y, oy):
            for k in range(4):
                t = (tp + k) % 4
                x_fwd_in(q, t).wait_recv()
                add_squares(q * 2 + oc, t)
        for q in range(2):
            for t in range(4):
                x_fwd(q, t).wait_send()
        total = jnp.sum(acc[...], axis=(0, 1), keepdims=True)
        inv = 1.0 / (jnp.sqrt(total) + NORM_EPS)

        @pl.loop(0, full_rows, step=16)
        def _(r):
            rr = pl.ds(pl.multiple_of(r, 16), 16)
            x[rr, :] = (x[rr, :].astype(F32) * inv).astype(BF16)

    blk = min(256, full_rows // 2)
    strips = full_rows // blk

    def mirror(dst, i, strip):
        for k in range(i + 1, strips):
            dst[k * blk:(k + 1) * blk, i * blk:(i + 1) * blk] = strip[:, (k - i) * blk:(k - i + 1) * blk].T

    def gram():
        for i in range(strips):
            lo = i * blk
            strip = lax.dot_general(x[lo:lo + blk, :], x[lo:, :], (((1,), (1,)), ((), ())),
                                    preferred_element_type=F32).astype(BF16)
            ga[lo:lo + blk, lo:] = strip
            mirror(ga, i, strip)

    def ns_poly():
        gram()
        for i in range(strips):
            lo = i * blk
            sq = jnp.dot(ga[lo:lo + blk, :], ga[:, lo:], preferred_element_type=F32)
            strip = (COEF_B * ga[lo:lo + blk, lo:].astype(F32) + COEF_C * sq).astype(BF16)
            gb[lo:lo + blk, lo:] = strip
            mirror(gb, i, strip)

    def ns_apply():
        cblk = ncol // 2

        @pl.loop(0, ncol, step=cblk)
        def _(r):
            rr = pl.ds(pl.multiple_of(r, cblk), cblk)
            prod = jnp.dot(gb[...], x[:, rr], preferred_element_type=F32)
            x[:, rr] = (COEF_A * x[:, rr].astype(F32) + prod).astype(BF16)

    def ns_last():
        gram()
        for q in range(2):
            part = ga[rowq(q * 2 + c), :]
            sq = jnp.dot(part, ga[...], preferred_element_type=F32)
            gb[q * rows:(q + 1) * rows, :] = (COEF_B * part.astype(F32) + COEF_C * sq).astype(BF16)

        @pl.loop(0, 4)
        def _(i):
            t = i + (3 - 2 * i) * (1 - tp // 2)
            prod = jnp.dot(gb[:2 * rows, :], x[:, colq(t)], preferred_element_type=F32)
            for q in range(2):
                rr = rowq(q * 2 + c)
                x[rr, colq(t)] = (COEF_A * x[rr, colq(t)].astype(F32)
                                  + prod[q * rows:(q + 1) * rows, :]).astype(BF16)
            send_back(y, t)

        @pl.when(mine >= 2)
        def _():
            send_cross()

    def x_send(q, t):
        return remote(x.at[rowq(q * 2 + c), colq(t)], xr.at[mine], s_xs.at[q, t], s_xr.at[mine], t, q * 2 + c)

    def x_recv(m):
        return remote(x.at[rowq(c), colq(0)], xr.at[m], s_xs.at[0, 0], s_xr.at[m], tp, dp_core)

    def send_back(q, t):
        @pl.when(jnp.logical_or(y != q, tp != t))
        def _():
            x_send(q, t).start()

        @pl.when(jnp.logical_and(y == q, tp == t))
        def _():
            xr[mine] = x[rowq(q * 2 + c), colq(t)]

    def send_cross():
        @pl.loop(0, 4)
        def _(i):
            send_back(oy, i + (3 - 2 * i) * (1 - tp // 2))

    def wb_send(m, ss, rs, rows_id, dp_id):
        part = wb.at[m, rowq(rows_id), :]
        return remote(part, part, ss.at[m], rs.at[m], tp, dp_id)

    def wb_core(m):
        return wb_send(m, s_ps, s_pr, dp, dp_core)

    def wb_core_in(m):
        return wb_send(m, s_ps, s_pr, dp_core, dp_core)

    def wb_y(m):
        return wb_send(m, s_gs, s_gr, dp, dp_y)

    def wb_y_in(m):
        return wb_send(m, s_gs, s_gr, dp_y, dp_y)

    def fwd_core(m):
        return wb_send(m, s_qs, s_qr, dp_y, dp_core)

    def fwd_core_in(m):
        return wb_send(m, s_qs, s_qr, oy * 2 + oc, dp_core)

    def update(m):
        @pl.when(mine != m)
        def _():
            x_recv(m).wait_recv()
        wt_copy(m).wait()
        rate = lr_ref[m]
        decay = decay_ref[0]

        @pl.loop(0, rows, step=16)
        def _(r):
            rr = pl.ds(pl.multiple_of(r, 16), 16)
            w = wt[m, rr, :]
            w = w - rate * (out_scale * xr[m, rr, :].astype(F32) + decay * w)
            wt[m, rr, :] = w
            wb[m, pl.ds(pl.multiple_of(dp * rows + r, 16), 16), :] = w.astype(BF16)
        wb_y(m).start()
        wb_core(m).start()

    def forward(m):
        wb_y_in(m).wait_recv()
        fwd_core(m).start()

    first_ns = mine + 4 - jnp.where(mine < 2, 1, 0)

    def halves_before(t):
        done = 2 * (t - first_ns)
        for until in FAST_SLOTS:
            done = done + jnp.maximum(jnp.minimum(t, until) - first_ns, 0)
        return jnp.minimum(jnp.maximum(done, 0), 2 * NS_STEPS)

    sum_cores(0)

    @pl.loop(0, mats + LATE + LAG_FWD)
    def _(t):
        @pl.when(t < mats - AHEAD)
        def _():
            issue(t + AHEAD, False)

        @pl.when(jnp.logical_and(t >= 1, t < mats + 1))
        def _():
            sum_y(t - 1)

        @pl.when(t < mats - 1)
        def _():
            sum_cores(t + 1)

        @pl.when(jnp.logical_and(t >= 2, t < mats + 2))
        def _():
            hop(t - 2)

        @pl.when(jnp.logical_and(t == CROSS_SLOT, mine < 2))
        def _():
            send_cross()

        @pl.when(t == EARLY)
        def _():
            @pl.loop(0, 2)
            def _(m):
                update(m)

        @pl.when(t == LATE + mine // 6 + mine // 7)
        def _():
            update(2)

        late = LATE - 1 + mine // 7

        @pl.when(jnp.logical_and(t >= late + 3, t < late + mats))
        def _():
            update(t - late)

        @pl.when(t >= LATE + LAG_FWD)
        def _():
            forward(t - LATE - LAG_FWD)

        @pl.when(t == first_ns)
        def _():
            gather_x()

        begin = halves_before(t)
        end = halves_before(t + 1)

        @pl.loop(begin, jnp.minimum(end, 2 * NS_STEPS - 2))
        def _(i):
            @pl.when(i % 2 == 0)
            def _():
                ns_poly()

            @pl.when(i % 2 == 1)
            def _():
                ns_apply()

        @pl.when(jnp.logical_and(begin < 2 * NS_STEPS, end == 2 * NS_STEPS))
        def _():
            ns_last()

    @pl.loop(0, mats)
    def _(j):
        for q in range(2):
            core_send(j, q).wait_send()
        y_send(j).wait_send()

        otp, oyy = owner_of(j)

        direct = is_direct(j)

        @pl.when(jnp.logical_or(jnp.logical_and(mine != j, y == oyy), jnp.logical_and(y != oyy, direct == 1)))
        def _():
            u_send(j, tp, dp_core).wait_send()

        @pl.when(jnp.logical_and(jnp.logical_and(mine != j, y == oyy), direct == 0))
        def _():
            u_pass(j, tp, dp_core).wait_send()

        @pl.when(jnp.logical_and(y != oyy, direct == 0))
        def _():
            u_cross(j).wait_send()
        wb_core(j).wait_send()
        wb_core_in(j).wait_recv()
        wb_y(j).wait_send()
        fwd_core(j).wait_send()
        fwd_core_in(j).wait_recv()
    for q in range(2):
        for t in range(4):
            @pl.when(jnp.logical_or(y != q, tp != t))
            def _():
                x_send(q, t).wait_send()


def solution(mesh):
    dp_size = mesh.shape["dp"]
    tp_size = mesh.shape["tp"]

    def local_step(grad_local, mom_local, weight_local, learn_rate, decay_rate):
        mats, rows, cols = mom_local.shape
        ncol = cols * tp_size
        nrow = rows * dp_size
        cfg = (mats, rows, cols, ncol, 0.2 * math.sqrt(max(nrow, ncol)), 1.0 / dp_size)
        dma = pltpu.SemaphoreType.DMA
        smem = pl.BlockSpec(memory_space=pltpu.SMEM)
        hbm = pl.BlockSpec(memory_space=pl.ANY)
        vmem = pl.BlockSpec(memory_space=pltpu.VMEM)
        return pl.pallas_call(
            functools.partial(kernel, cfg),
            out_shape=(pltpu.VMEM((mats, rows, cols), F32),
                       pltpu.VMEM((mats, rows, cols), F32),
                       pltpu.VMEM((mats, nrow, cols), BF16)),
            in_specs=[smem, smem, hbm, hbm, hbm],
            out_specs=(vmem, vmem, vmem),
            scratch_shapes=[
                pltpu.VMEM((mats, 2, rows, cols), F32),
                pltpu.VMEM((mats, 2, rows, cols), F32),
                pltpu.VMEM((mats, rows, cols), F32),
                pltpu.VMEM((mats, rows, cols), BF16),
                pltpu.VMEM((nrow, ncol), BF16),
                pltpu.VMEM((nrow, nrow), BF16),
                pltpu.VMEM((nrow, nrow), BF16),
                pltpu.VMEM((mats, rows, cols), BF16),
                pltpu.VMEM((16, cols), F32),
                pltpu.VMEM((mats, rows, cols), BF16),
                dma((mats, 2)), dma((mats,)), dma((mats,)),
                dma((mats, 2)), dma((mats, 2)),
                dma((mats,)), dma((mats,)),
                dma((mats,)), dma((2, tp_size)),
                dma((2, tp_size)), dma((2, tp_size)),
                dma((2, tp_size)), dma((mats,)),
                dma((mats,)), dma((mats,)), dma((mats,)),
                dma((mats,)), dma((mats,)), dma((mats,)), dma((mats,)),
                dma((mats,)), dma((mats,)),
            ],
            compiler_params=pltpu.CompilerParams(
                collective_id=0, has_side_effects=True, vmem_limit_bytes=VMEM_MIB * 2 ** 20),
            name="muon_step",
        )(learn_rate, decay_rate.reshape(1), grad_local[0], mom_local, weight_local)

    return jax.shard_map(
        local_step,
        mesh=mesh,
        in_specs=(P(("rep", "dp"), None, None, "tp"), P("rep", "dp", "tp"), P("rep", "dp", "tp"), P("rep"), P()),
        out_specs=(P("rep", "dp", "tp"), P("rep", "dp", "tp"), P("rep", None, "tp")),
        check_vma=False,
    )
```

```python
import functools
import math
import jax
import jax.numpy as jnp
from jax import lax
from jax.experimental import pallas as pl
from jax.experimental.pallas import tpu as pltpu
from jax.sharding import PartitionSpec as P

MOMENTUM = 0.95
NS_STEPS = 5
COEF_A = 3.4445
COEF_B = -4.7750
COEF_C = 2.0315
NORM_EPS = 1e-7
MESH = pl.DeviceIdType.MESH
F32 = jnp.float32
BF16 = jnp.bfloat16

OWNERS = ((2, 0, 0), (1, 1, 0), (1, 0, 0), (2, 1, 0), (2, 0, 1), (1, 1, 1), (1, 0, 1), (2, 1, 1))
NOBODY = 100
AHEAD = 2
VMEM_MIB = 44
FAST_SLOTS = (6, 9)
FIRST_NS = 3
CROSS_SLOT = 9
EARLY = 10
LATE = 13
LAG_FWD = 3


def owner_of(j):
    tp, y, core = 0, 0, 0
    for k, (tp_k, y_k, core_k) in enumerate(OWNERS):
        tp = tp + jnp.where(j == k, tp_k, 0)
        y = y + jnp.where(j == k, y_k, 0)
        core = core + jnp.where(j == k, core_k, 0)
    return tp, y, y * 2 + core


def matrix_of(tp, y, core):
    mine = NOBODY
    for k, (tp_k, y_k, core_k) in enumerate(OWNERS):
        here = jnp.logical_and(tp == tp_k, jnp.logical_and(y == y_k, core == core_k))
        mine = mine - jnp.where(here, NOBODY - k, 0)
    return mine


def kernel(cfg, lr_ref, decay_ref, grad, mom_in, wt_in, mom, wt, wb,
           own, rcv, yr, ub, x, ga, gb, uf, acc, xr,
           s_own, s_mom, s_wt, s_c2s, s_c2r, s_ys, s_yr, s_us, s_ur, s_xs, s_xr,
           s_hs, s_hr, s_vs, s_ps, s_pr, s_gs, s_gr, s_qs, s_qr):
    mats, rows, cols, ncol, out_scale, inv_dp = cfg
    full_rows = 4 * rows
    tp = lax.axis_index("tp")
    dp = lax.axis_index("dp")
    y = dp // 2
    c = dp % 2
    oy = 1 - y
    oc = 1 - c
    dp_core = y * 2 + oc
    dp_y = oy * 2 + c
    mine = matrix_of(tp, y, c)

    def rowq(q):
        return pl.ds(pl.multiple_of(q * rows, rows), rows)

    def colq(t):
        return pl.ds(pl.multiple_of(t * cols, cols), cols)

    def remote(src, dst, ss, rs, tp_id, dp_id):
        return pltpu.make_async_remote_copy(
            src_ref=src, dst_ref=dst, send_sem=ss, recv_sem=rs,
            device_id={"tp": tp_id, "dp": dp_id}, device_id_type=MESH)

    def own_copy(j, q):
        return pltpu.make_async_copy(grad.at[j, rowq(q * 2 + c), :], own.at[j, q], s_own.at[j, q])

    def mom_copy(j):
        return pltpu.make_async_copy(mom_in.at[j], mom.at[j], s_mom.at[j])

    def wt_copy(j):
        return pltpu.make_async_copy(wt_in.at[j], wt.at[j], s_wt.at[j])

    def core_send(j, q):
        return remote(grad.at[j, rowq(q * 2 + oc), :], rcv.at[j, q], s_c2s.at[j, q], s_c2r.at[j, q], tp, dp_core)

    barrier = pltpu.get_barrier_semaphore()
    for k in range(1, 16):
        tgt = (tp * 4 + dp + k) % 16
        pl.semaphore_signal(barrier, inc=1, device_id={"tp": tgt // 4, "dp": tgt % 4}, device_id_type=MESH)
    own_copy(0, oy).start()
    pl.semaphore_wait(barrier, 15)

    def issue(j, first):
        core_send(j, oy).start()
        if not first:
            own_copy(j, oy).start()
        core_send(j, y).start()
        own_copy(j, y).start()
        mom_copy(j).start()

    for j in range(AHEAD):
        issue(j, j == 0)

    def y_send(j):
        return remote(own.at[j, oy], yr.at[j], s_ys.at[j], s_yr.at[j], tp, dp_y)

    def sum_cores(j):
        own_copy(j, oy).wait()
        core_send(j, oy).wait_recv()

        @pl.loop(0, rows, step=16)
        def _(r):
            rr = pl.ds(pl.multiple_of(r, 16), 16)
            own[j, oy, rr, :] = own[j, oy, rr, :] + rcv[j, oy, rr, :]
        y_send(j).start()

    def u_send(j, tp_id, dp_id):
        return remote(ub.at[j], x.at[rowq(dp), colq(tp)], s_us.at[j], s_ur.at[dp, tp], tp_id, dp_id)

    def sum_y(j):
        own_copy(j, y).wait()
        core_send(j, y).wait_recv()
        mom_copy(j).wait()
        y_send(j).wait_recv()

        @pl.loop(0, rows, step=16)
        def _(r):
            rr = pl.ds(pl.multiple_of(r, 16), 16)
            g = (own[j, y, rr, :] + rcv[j, y, rr, :] + yr[j, rr, :]) * inv_dp
            m = MOMENTUM * mom[j, rr, :] + g
            mom[j, rr, :] = m
            ub[j, rr, :] = (g + MOMENTUM * m).astype(BF16)
        wt_copy(j).start()
        otp, oyy, odp = owner_of(j)

        @pl.when(mine == j)
        def _():
            x[rowq(dp), colq(tp)] = ub[j]

        @pl.when(jnp.logical_and(mine != j, y == oyy))
        def _():
            u_send(j, otp, odp).start()

        @pl.when(y != oyy)
        def _():
            u_cross(j).start()

    def u_cross(j):
        return remote(ub.at[j], uf.at[j], s_hs.at[j], s_hr.at[j], tp, dp_y)

    def u_pass(j, tp_id, dp_id):
        return remote(uf.at[j], x.at[rowq(dp_y), colq(tp)], s_vs.at[j], s_ur.at[dp_y, tp], tp_id, dp_id)

    def hop(j):
        otp, oyy, odp = owner_of(j)

        @pl.when(y == oyy)
        def _():
            u_cross(j).wait_recv()

            @pl.when(mine == j)
            def _():
                x[rowq(dp_y), colq(tp)] = uf[j]

            @pl.when(mine != j)
            def _():
                u_pass(j, otp, odp).start()

    def piece(q, t):
        return remote(ub.at[0], x.at[rowq(q), colq(t)], s_us.at[0], s_ur.at[q, t], tp, dp_core)

    def add_squares(q, t):
        def body(i, carry):
            v = x[pl.ds(pl.multiple_of(q * rows + i * 16, 16), 16), colq(t)].astype(F32)
            return carry + v * v
        acc[...] = lax.fori_loop(0, rows // 16, body, acc[...])

    def gather_x():
        acc[...] = jnp.zeros_like(acc)
        for part, q in enumerate((dp, dp_core, dp_y, oy * 2 + oc)):
            @pl.loop(0, 4)
            def _(k):
                t = (tp + k) % 4

                @pl.when(k >= 1 - part % 2)
                def _():
                    piece(q, t).wait_recv()
                add_squares(q, t)
        total = jnp.sum(acc[...], axis=(0, 1), keepdims=True)
        inv = 1.0 / (jnp.sqrt(total) + NORM_EPS)

        @pl.loop(0, full_rows, step=16)
        def _(r):
            rr = pl.ds(pl.multiple_of(r, 16), 16)
            x[rr, :] = (x[rr, :].astype(F32) * inv).astype(BF16)

    blk = min(256, full_rows // 2)
    strips = full_rows // blk

    def mirror(dst, i, strip):
        for k in range(i + 1, strips):
            dst[k * blk:(k + 1) * blk, i * blk:(i + 1) * blk] = strip[:, (k - i) * blk:(k - i + 1) * blk].T

    def gram():
        for i in range(strips):
            lo = i * blk
            strip = lax.dot_general(x[lo:lo + blk, :], x[lo:, :], (((1,), (1,)), ((), ())),
                                    preferred_element_type=F32).astype(BF16)
            ga[lo:lo + blk, lo:] = strip
            mirror(ga, i, strip)

    def ns_poly():
        gram()
        for i in range(strips):
            lo = i * blk
            sq = jnp.dot(ga[lo:lo + blk, :], ga[:, lo:], preferred_element_type=F32)
            strip = (COEF_B * ga[lo:lo + blk, lo:].astype(F32) + COEF_C * sq).astype(BF16)
            gb[lo:lo + blk, lo:] = strip
            mirror(gb, i, strip)

    def ns_apply():
        cblk = ncol // 2

        @pl.loop(0, ncol, step=cblk)
        def _(r):
            rr = pl.ds(pl.multiple_of(r, cblk), cblk)
            prod = jnp.dot(gb[...], x[:, rr], preferred_element_type=F32)
            x[:, rr] = (COEF_A * x[:, rr].astype(F32) + prod).astype(BF16)

    def ns_last():
        ns_poly()

        @pl.loop(0, 4)
        def _(i):
            t = i + (3 - 2 * i) * (1 - tp // 2)
            prod = jnp.dot(gb[...], x[:, colq(t)], preferred_element_type=F32)
            x[:, colq(t)] = (COEF_A * x[:, colq(t)].astype(F32) + prod).astype(BF16)
            for k in range(2):
                send_back(y * 2 + k, t)

        @pl.when(mine >= 2)
        def _():
            send_cross()

    def x_send(q, t):
        return remote(x.at[rowq(q), colq(t)], xr.at[mine], s_xs.at[q, t], s_xr.at[mine], t, q)

    def x_recv(m):
        return remote(x.at[rowq(c), colq(0)], xr.at[m], s_xs.at[0, 0], s_xr.at[m], tp, dp_core)

    def send_back(q, t):
        @pl.when(jnp.logical_or(dp != q, tp != t))
        def _():
            x_send(q, t).start()

        @pl.when(jnp.logical_and(dp == q, tp == t))
        def _():
            xr[mine] = x[rowq(dp), colq(t)]

    def send_cross():
        @pl.loop(0, 4)
        def _(i):
            for k in range(2):
                send_back(oy * 2 + k, i + (3 - 2 * i) * (1 - tp // 2))

    def wb_send(m, ss, rs, rows_id, dp_id):
        part = wb.at[m, rowq(rows_id), :]
        return remote(part, part, ss.at[m], rs.at[m], tp, dp_id)

    def wb_core(m):
        return wb_send(m, s_ps, s_pr, dp, dp_core)

    def wb_core_in(m):
        return wb_send(m, s_ps, s_pr, dp_core, dp_core)

    def wb_y(m):
        return wb_send(m, s_gs, s_gr, dp, dp_y)

    def wb_y_in(m):
        return wb_send(m, s_gs, s_gr, dp_y, dp_y)

    def fwd_core(m):
        return wb_send(m, s_qs, s_qr, dp_y, dp_core)

    def fwd_core_in(m):
        return wb_send(m, s_qs, s_qr, oy * 2 + oc, dp_core)

    def update(m):
        @pl.when(mine != m)
        def _():
            x_recv(m).wait_recv()
        wt_copy(m).wait()
        rate = lr_ref[m]
        decay = decay_ref[0]

        @pl.loop(0, rows, step=16)
        def _(r):
            rr = pl.ds(pl.multiple_of(r, 16), 16)
            w = wt[m, rr, :]
            w = w - rate * (out_scale * xr[m, rr, :].astype(F32) + decay * w)
            wt[m, rr, :] = w
            wb[m, pl.ds(pl.multiple_of(dp * rows + r, 16), 16), :] = w.astype(BF16)
        wb_y(m).start()
        wb_core(m).start()

    def forward(m):
        wb_y_in(m).wait_recv()
        fwd_core(m).start()

    first_ns = mine + FIRST_NS + jnp.where(mine > 5, 1, 0)
    is_6 = jnp.where(mine == 6, 1, 0)
    is_7 = jnp.where(mine == 7, 1, 0)

    def halves_before(t):
        done = 2 * (t - first_ns)
        for until in FAST_SLOTS:
            done = done + jnp.maximum(jnp.minimum(t, until) - first_ns, 0)
        return jnp.minimum(jnp.maximum(done, 0), 2 * NS_STEPS)

    sum_cores(0)

    @pl.loop(0, mats + LATE + LAG_FWD)
    def _(t):
        @pl.when(t < mats - AHEAD)
        def _():
            issue(t + AHEAD, False)

        @pl.when(jnp.logical_and(t >= 1, t < mats + 1))
        def _():
            sum_y(t - 1)

        @pl.when(t < mats - 1)
        def _():
            sum_cores(t + 1)

        @pl.when(jnp.logical_and(t >= 2, t < mats + 2))
        def _():
            hop(t - 2)

        @pl.when(jnp.logical_and(t == CROSS_SLOT, mine < 2))
        def _():
            send_cross()

        @pl.when(t == EARLY)
        def _():
            @pl.loop(0, 2)
            def _(m):
                update(m)

        @pl.when(t == LATE + is_6 + 2 * is_7)
        def _():
            update(2)

        late = LATE - 1 + is_7

        @pl.when(jnp.logical_and(t >= late + 3, t < late + mats))
        def _():
            update(t - late)

        @pl.when(t >= LATE + LAG_FWD)
        def _():
            forward(t - LATE - LAG_FWD)

        @pl.when(t == first_ns)
        def _():
            gather_x()

        begin = halves_before(t)
        end = halves_before(t + 1)

        @pl.loop(begin, jnp.minimum(end, 2 * NS_STEPS - 2))
        def _(i):
            @pl.when(i % 2 == 0)
            def _():
                ns_poly()

            @pl.when(i % 2 == 1)
            def _():
                ns_apply()

        @pl.when(jnp.logical_and(begin < 2 * NS_STEPS, end == 2 * NS_STEPS))
        def _():
            ns_last()

    @pl.loop(0, mats)
    def _(j):
        for q in range(2):
            core_send(j, q).wait_send()
        y_send(j).wait_send()

        otp, oyy, odp = owner_of(j)

        @pl.when(jnp.logical_and(mine != j, y == oyy))
        def _():
            u_send(j, tp, dp_core).wait_send()
            u_pass(j, tp, dp_core).wait_send()

        @pl.when(y != oyy)
        def _():
            u_cross(j).wait_send()
        wb_core(j).wait_send()
        wb_core_in(j).wait_recv()
        wb_y(j).wait_send()
        fwd_core(j).wait_send()
        fwd_core_in(j).wait_recv()

    @pl.when(mine < mats)
    def _():
        for q in range(4):
            for t in range(4):
                @pl.when(jnp.logical_or(dp != q, tp != t))
                def _():
                    x_send(q, t).wait_send()


def solution(mesh):
    dp_size = mesh.shape["dp"]
    tp_size = mesh.shape["tp"]

    def local_step(grad_local, mom_local, weight_local, learn_rate, decay_rate):
        mats, rows, cols = mom_local.shape
        ncol = cols * tp_size
        nrow = rows * dp_size
        cfg = (mats, rows, cols, ncol, 0.2 * math.sqrt(max(nrow, ncol)), 1.0 / dp_size)
        dma = pltpu.SemaphoreType.DMA
        smem = pl.BlockSpec(memory_space=pltpu.SMEM)
        hbm = pl.BlockSpec(memory_space=pl.ANY)
        vmem = pl.BlockSpec(memory_space=pltpu.VMEM)
        return pl.pallas_call(
            functools.partial(kernel, cfg),
            out_shape=(pltpu.VMEM((mats, rows, cols), F32),
                       pltpu.VMEM((mats, rows, cols), F32),
                       pltpu.VMEM((mats, nrow, cols), BF16)),
            in_specs=[smem, smem, hbm, hbm, hbm],
            out_specs=(vmem, vmem, vmem),
            scratch_shapes=[
                pltpu.VMEM((mats, 2, rows, cols), F32),
                pltpu.VMEM((mats, 2, rows, cols), F32),
                pltpu.VMEM((mats, rows, cols), F32),
                pltpu.VMEM((mats, rows, cols), BF16),
                pltpu.VMEM((nrow, ncol), BF16),
                pltpu.VMEM((nrow, nrow), BF16),
                pltpu.VMEM((nrow, nrow), BF16),
                pltpu.VMEM((mats, rows, cols), BF16),
                pltpu.VMEM((16, cols), F32),
                pltpu.VMEM((mats, rows, cols), BF16),
                dma((mats, 2)), dma((mats,)), dma((mats,)),
                dma((mats, 2)), dma((mats, 2)),
                dma((mats,)), dma((mats,)),
                dma((mats,)), dma((dp_size, tp_size)),
                dma((dp_size, tp_size)), dma((mats,)),
                dma((mats,)), dma((mats,)), dma((mats,)),
                dma((mats,)), dma((mats,)), dma((mats,)), dma((mats,)),
                dma((mats,)), dma((mats,)),
            ],
            compiler_params=pltpu.CompilerParams(
                collective_id=0, has_side_effects=True, vmem_limit_bytes=VMEM_MIB * 2 ** 20),
            name="muon_step",
        )(learn_rate, decay_rate.reshape(1), grad_local[0], mom_local, weight_local)

    return jax.shard_map(
        local_step,
        mesh=mesh,
        in_specs=(P(("rep", "dp"), None, None, "tp"), P("rep", "dp", "tp"), P("rep", "dp", "tp"), P("rep"), P()),
        out_specs=(P("rep", "dp", "tp"), P("rep", "dp", "tp"), P("rep", None, "tp")),
        check_vma=False,
    )
```

```python
import functools
import math
import jax
import jax.numpy as jnp
from jax import lax
from jax.experimental import pallas as pl
from jax.experimental.pallas import tpu as pltpu
from jax.sharding import PartitionSpec as P

MOMENTUM = 0.95
NS_STEPS = 5
COEF_A = 3.4445
COEF_B = -4.7750
COEF_C = 2.0315
NORM_EPS = 1e-7
MESH = pl.DeviceIdType.MESH
F32 = jnp.float32
BF16 = jnp.bfloat16

OWNERS = ((2, 0, 0), (1, 1, 0), (1, 0, 0), (2, 1, 0), (2, 0, 1), (1, 1, 1), (1, 0, 1), (2, 1, 1))
NOBODY = 100
AHEAD = 2
VMEM_MIB = 44
FAST_SLOTS = (6, 9)
FIRST_NS = 3
CROSS_SLOT = 9
EARLY = 10
LATE = 13
LAG_FWD = 3


def owner_of(j):
    tp, y, core = 0, 0, 0
    for k, (tp_k, y_k, core_k) in enumerate(OWNERS):
        tp = tp + jnp.where(j == k, tp_k, 0)
        y = y + jnp.where(j == k, y_k, 0)
        core = core + jnp.where(j == k, core_k, 0)
    return tp, y, y * 2 + core


def matrix_of(tp, y, core):
    mine = NOBODY
    for k, (tp_k, y_k, core_k) in enumerate(OWNERS):
        here = jnp.logical_and(tp == tp_k, jnp.logical_and(y == y_k, core == core_k))
        mine = mine - jnp.where(here, NOBODY - k, 0)
    return mine


def kernel(cfg, lr_ref, decay_ref, grad, mom_in, wt_in, mom, wt, wb,
           own, rcv, yr, ub, x, ga, gb, uf, acc, xr,
           s_own, s_mom, s_wt, s_c2s, s_c2r, s_ys, s_yr, s_us, s_ur, s_xs, s_xr,
           s_hs, s_hr, s_vs, s_ps, s_pr, s_gs, s_gr, s_qs, s_qr):
    mats, rows, cols, ncol, out_scale, inv_dp = cfg
    full_rows = 4 * rows
    tp = lax.axis_index("tp")
    dp = lax.axis_index("dp")
    y = dp // 2
    c = dp % 2
    oy = 1 - y
    oc = 1 - c
    dp_core = y * 2 + oc
    dp_y = oy * 2 + c
    mine = matrix_of(tp, y, c)

    def rowq(q):
        return pl.ds(pl.multiple_of(q * rows, rows), rows)

    def colq(t):
        return pl.ds(pl.multiple_of(t * cols, cols), cols)

    def remote(src, dst, ss, rs, tp_id, dp_id):
        return pltpu.make_async_remote_copy(
            src_ref=src, dst_ref=dst, send_sem=ss, recv_sem=rs,
            device_id={"tp": tp_id, "dp": dp_id}, device_id_type=MESH)

    def own_copy(j, q):
        return pltpu.make_async_copy(grad.at[j, rowq(q * 2 + c), :], own.at[j, q], s_own.at[j, q])

    def mom_copy(j):
        return pltpu.make_async_copy(mom_in.at[j], mom.at[j], s_mom.at[j])

    def wt_copy(j):
        return pltpu.make_async_copy(wt_in.at[j], wt.at[j], s_wt.at[j])

    def core_send(j, q):
        return remote(grad.at[j, rowq(q * 2 + oc), :], rcv.at[j, q], s_c2s.at[j, q], s_c2r.at[j, q], tp, dp_core)

    barrier = pltpu.get_barrier_semaphore()
    for k in range(1, 16):
        tgt = (tp * 4 + dp + k) % 16
        pl.semaphore_signal(barrier, inc=1, device_id={"tp": tgt // 4, "dp": tgt % 4}, device_id_type=MESH)
    own_copy(0, oy).start()
    pl.semaphore_wait(barrier, 15)

    def issue(j, first):
        core_send(j, oy).start()
        if not first:
            own_copy(j, oy).start()
        core_send(j, y).start()
        own_copy(j, y).start()
        mom_copy(j).start()

    for j in range(AHEAD):
        issue(j, j == 0)

    def y_send(j):
        return remote(own.at[j, oy], yr.at[j], s_ys.at[j], s_yr.at[j], tp, dp_y)

    def sum_cores(j):
        own_copy(j, oy).wait()
        core_send(j, oy).wait_recv()

        @pl.loop(0, rows, step=16)
        def _(r):
            rr = pl.ds(pl.multiple_of(r, 16), 16)
            own[j, oy, rr, :] = own[j, oy, rr, :] + rcv[j, oy, rr, :]
        y_send(j).start()

    def u_send(j, tp_id, dp_id):
        return remote(ub.at[j], x.at[rowq(dp), colq(tp)], s_us.at[j], s_ur.at[dp, tp], tp_id, dp_id)

    def sum_y(j):
        own_copy(j, y).wait()
        core_send(j, y).wait_recv()
        mom_copy(j).wait()
        y_send(j).wait_recv()

        @pl.loop(0, rows, step=16)
        def _(r):
            rr = pl.ds(pl.multiple_of(r, 16), 16)
            g = (own[j, y, rr, :] + rcv[j, y, rr, :] + yr[j, rr, :]) * inv_dp
            m = MOMENTUM * mom[j, rr, :] + g
            mom[j, rr, :] = m
            ub[j, rr, :] = (g + MOMENTUM * m).astype(BF16)
        wt_copy(j).start()
        otp, oyy, odp = owner_of(j)

        @pl.when(mine == j)
        def _():
            x[rowq(dp), colq(tp)] = ub[j]

        @pl.when(jnp.logical_and(mine != j, y == oyy))
        def _():
            u_send(j, otp, odp).start()

        @pl.when(y != oyy)
        def _():
            u_cross(j).start()

    def u_cross(j):
        return remote(ub.at[j], uf.at[j], s_hs.at[j], s_hr.at[j], tp, dp_y)

    def u_pass(j, tp_id, dp_id):
        return remote(uf.at[j], x.at[rowq(dp_y), colq(tp)], s_vs.at[j], s_ur.at[dp_y, tp], tp_id, dp_id)

    def hop(j):
        otp, oyy, odp = owner_of(j)

        @pl.when(y == oyy)
        def _():
            u_cross(j).wait_recv()

            @pl.when(mine == j)
            def _():
                x[rowq(dp_y), colq(tp)] = uf[j]

            @pl.when(mine != j)
            def _():
                u_pass(j, otp, odp).start()

    def piece(q, t):
        return remote(ub.at[0], x.at[rowq(q), colq(t)], s_us.at[0], s_ur.at[q, t], tp, dp_core)

    def add_squares(q, t):
        def body(i, carry):
            v = x[pl.ds(pl.multiple_of(q * rows + i * 16, 16), 16), colq(t)].astype(F32)
            return carry + v * v
        acc[...] = lax.fori_loop(0, rows // 16, body, acc[...])

    def gather_x():
        acc[...] = jnp.zeros_like(acc)
        for part, q in enumerate((dp, dp_core, dp_y, oy * 2 + oc)):
            @pl.loop(0, 4)
            def _(k):
                t = (tp + k) % 4

                @pl.when(k >= 1 - part % 2)
                def _():
                    piece(q, t).wait_recv()
                add_squares(q, t)
        total = jnp.sum(acc[...], axis=(0, 1), keepdims=True)
        inv = 1.0 / (jnp.sqrt(total) + NORM_EPS)

        @pl.loop(0, full_rows, step=16)
        def _(r):
            rr = pl.ds(pl.multiple_of(r, 16), 16)
            x[rr, :] = (x[rr, :].astype(F32) * inv).astype(BF16)

    blk = min(256, full_rows // 2)
    strips = full_rows // blk

    def mirror(dst, i, strip):
        for k in range(i + 1, strips):
            dst[k * blk:(k + 1) * blk, i * blk:(i + 1) * blk] = strip[:, (k - i) * blk:(k - i + 1) * blk].T

    def gram():
        for i in range(strips):
            lo = i * blk
            strip = lax.dot_general(x[lo:lo + blk, :], x[lo:, :], (((1,), (1,)), ((), ())),
                                    preferred_element_type=F32).astype(BF16)
            ga[lo:lo + blk, lo:] = strip
            mirror(ga, i, strip)

    def ns_poly():
        gram()
        for i in range(strips):
            lo = i * blk
            sq = jnp.dot(ga[lo:lo + blk, :], ga[:, lo:], preferred_element_type=F32)
            strip = (COEF_B * ga[lo:lo + blk, lo:].astype(F32) + COEF_C * sq).astype(BF16)
            gb[lo:lo + blk, lo:] = strip
            mirror(gb, i, strip)

    def ns_apply():
        cblk = ncol // 2

        @pl.loop(0, ncol, step=cblk)
        def _(r):
            rr = pl.ds(pl.multiple_of(r, cblk), cblk)
            prod = jnp.dot(gb[...], x[:, rr], preferred_element_type=F32)
            x[:, rr] = (COEF_A * x[:, rr].astype(F32) + prod).astype(BF16)

    def ns_last():
        ns_poly()

        @pl.loop(0, 4)
        def _(i):
            t = i + (3 - 2 * i) * (1 - tp // 2)
            prod = jnp.dot(gb[...], x[:, colq(t)], preferred_element_type=F32)
            x[:, colq(t)] = (COEF_A * x[:, colq(t)].astype(F32) + prod).astype(BF16)
            for k in range(2):
                send_back(y * 2 + k, t)

        @pl.when(mine >= 2)
        def _():
            send_cross()

    def x_send(q, t):
        return remote(x.at[rowq(q), colq(t)], xr.at[mine], s_xs.at[q, t], s_xr.at[mine], t, q)

    def x_recv(m):
        return remote(x.at[rowq(c), colq(0)], xr.at[m], s_xs.at[0, 0], s_xr.at[m], tp, dp_core)

    def send_back(q, t):
        @pl.when(jnp.logical_or(dp != q, tp != t))
        def _():
            x_send(q, t).start()

        @pl.when(jnp.logical_and(dp == q, tp == t))
        def _():
            xr[mine] = x[rowq(dp), colq(t)]

    def send_cross():
        @pl.loop(0, 4)
        def _(i):
            for k in range(2):
                send_back(oy * 2 + k, i + (3 - 2 * i) * (1 - tp // 2))

    def wb_send(m, ss, rs, rows_id, dp_id):
        part = wb.at[m, rowq(rows_id), :]
        return remote(part, part, ss.at[m], rs.at[m], tp, dp_id)

    def wb_core(m):
        return wb_send(m, s_ps, s_pr, dp, dp_core)

    def wb_core_in(m):
        return wb_send(m, s_ps, s_pr, dp_core, dp_core)

    def wb_y(m):
        return wb_send(m, s_gs, s_gr, dp, dp_y)

    def wb_y_in(m):
        return wb_send(m, s_gs, s_gr, dp_y, dp_y)

    def fwd_core(m):
        return wb_send(m, s_qs, s_qr, dp_y, dp_core)

    def fwd_core_in(m):
        return wb_send(m, s_qs, s_qr, oy * 2 + oc, dp_core)

    def update(m):
        @pl.when(mine != m)
        def _():
            x_recv(m).wait_recv()
        wt_copy(m).wait()
        rate = lr_ref[m]
        decay = decay_ref[0]

        @pl.loop(0, rows, step=16)
        def _(r):
            rr = pl.ds(pl.multiple_of(r, 16), 16)
            w = wt[m, rr, :]
            w = w - rate * (out_scale * xr[m, rr, :].astype(F32) + decay * w)
            wt[m, rr, :] = w
            wb[m, pl.ds(pl.multiple_of(dp * rows + r, 16), 16), :] = w.astype(BF16)
        wb_y(m).start()
        wb_core(m).start()

    def forward(m):
        wb_y_in(m).wait_recv()
        fwd_core(m).start()

    first_ns = mine + FIRST_NS + jnp.where(mine > 5, 1, 0)
    is_6 = jnp.where(mine == 6, 1, 0)
    is_7 = jnp.where(mine == 7, 1, 0)
    early = EARLY + 2 * jnp.where(jnp.logical_and(mine >= 4, mine < 7), 1, 0)

    def halves_before(t):
        done = 2 * (t - first_ns)
        for until in FAST_SLOTS:
            done = done + jnp.maximum(jnp.minimum(t, until) - first_ns, 0)
        return jnp.minimum(jnp.maximum(done, 0), 2 * NS_STEPS)

    sum_cores(0)

    @pl.loop(0, mats + LATE + LAG_FWD)
    def _(t):
        @pl.when(t < mats - AHEAD)
        def _():
            issue(t + AHEAD, False)

        @pl.when(jnp.logical_and(t >= 1, t < mats + 1))
        def _():
            sum_y(t - 1)

        @pl.when(t < mats - 1)
        def _():
            sum_cores(t + 1)

        @pl.when(jnp.logical_and(t >= 2, t < mats + 2))
        def _():
            hop(t - 2)

        @pl.when(jnp.logical_and(t == CROSS_SLOT, mine < 2))
        def _():
            send_cross()

        @pl.when(t == early)
        def _():
            @pl.loop(0, 2)
            def _(m):
                update(m)

        @pl.when(t == LATE + is_6 + 2 * is_7)
        def _():
            update(2)

        late = LATE - 1 + is_7

        @pl.when(jnp.logical_and(t >= late + 3, t < late + mats))
        def _():
            update(t - late)

        @pl.when(t >= LATE + LAG_FWD)
        def _():
            forward(t - LATE - LAG_FWD)

        @pl.when(t == first_ns)
        def _():
            gather_x()

        begin = halves_before(t)
        end = halves_before(t + 1)

        @pl.loop(begin, jnp.minimum(end, 2 * NS_STEPS - 2))
        def _(i):
            @pl.when(i % 2 == 0)
            def _():
                ns_poly()

            @pl.when(i % 2 == 1)
            def _():
                ns_apply()

        @pl.when(jnp.logical_and(begin < 2 * NS_STEPS, end == 2 * NS_STEPS))
        def _():
            ns_last()

    @pl.loop(0, mats)
    def _(j):
        for q in range(2):
            core_send(j, q).wait_send()
        y_send(j).wait_send()

        otp, oyy, odp = owner_of(j)

        @pl.when(jnp.logical_and(mine != j, y == oyy))
        def _():
            u_send(j, tp, dp_core).wait_send()
            u_pass(j, tp, dp_core).wait_send()

        @pl.when(y != oyy)
        def _():
            u_cross(j).wait_send()
        wb_core(j).wait_send()
        wb_core_in(j).wait_recv()
        wb_y(j).wait_send()
        fwd_core(j).wait_send()
        fwd_core_in(j).wait_recv()

    @pl.when(mine < mats)
    def _():
        for q in range(4):
            for t in range(4):
                @pl.when(jnp.logical_or(dp != q, tp != t))
                def _():
                    x_send(q, t).wait_send()


def solution(mesh):
    dp_size = mesh.shape["dp"]
    tp_size = mesh.shape["tp"]

    def local_step(grad_local, mom_local, weight_local, learn_rate, decay_rate):
        mats, rows, cols = mom_local.shape
        ncol = cols * tp_size
        nrow = rows * dp_size
        cfg = (mats, rows, cols, ncol, 0.2 * math.sqrt(max(nrow, ncol)), 1.0 / dp_size)
        dma = pltpu.SemaphoreType.DMA
        smem = pl.BlockSpec(memory_space=pltpu.SMEM)
        hbm = pl.BlockSpec(memory_space=pl.ANY)
        vmem = pl.BlockSpec(memory_space=pltpu.VMEM)
        return pl.pallas_call(
            functools.partial(kernel, cfg),
            out_shape=(pltpu.VMEM((mats, rows, cols), F32),
                       pltpu.VMEM((mats, rows, cols), F32),
                       pltpu.VMEM((mats, nrow, cols), BF16)),
            in_specs=[smem, smem, hbm, hbm, hbm],
            out_specs=(vmem, vmem, vmem),
            scratch_shapes=[
                pltpu.VMEM((mats, 2, rows, cols), F32),
                pltpu.VMEM((mats, 2, rows, cols), F32),
                pltpu.VMEM((mats, rows, cols), F32),
                pltpu.VMEM((mats, rows, cols), BF16),
                pltpu.VMEM((nrow, ncol), BF16),
                pltpu.VMEM((nrow, nrow), BF16),
                pltpu.VMEM((nrow, nrow), BF16),
                pltpu.VMEM((mats, rows, cols), BF16),
                pltpu.VMEM((16, cols), F32),
                pltpu.VMEM((mats, rows, cols), BF16),
                dma((mats, 2)), dma((mats,)), dma((mats,)),
                dma((mats, 2)), dma((mats, 2)),
                dma((mats,)), dma((mats,)),
                dma((mats,)), dma((dp_size, tp_size)),
                dma((dp_size, tp_size)), dma((mats,)),
                dma((mats,)), dma((mats,)), dma((mats,)),
                dma((mats,)), dma((mats,)), dma((mats,)), dma((mats,)),
                dma((mats,)), dma((mats,)),
            ],
            compiler_params=pltpu.CompilerParams(
                collective_id=0, has_side_effects=True, vmem_limit_bytes=VMEM_MIB * 2 ** 20),
            name="muon_step",
        )(learn_rate, decay_rate.reshape(1), grad_local[0], mom_local, weight_local)

    return jax.shard_map(
        local_step,
        mesh=mesh,
        in_specs=(P(("rep", "dp"), None, None, "tp"), P("rep", "dp", "tp"), P("rep", "dp", "tp"), P("rep"), P()),
        out_specs=(P("rep", "dp", "tp"), P("rep", "dp", "tp"), P("rep", None, "tp")),
        check_vma=False,
    )
```
